32 devices in a mesh: scen: 8 (over z, core), grp: 4 (over y, x).
Axes of the slice: x: 2, y: 2, z: 4, core: 2. Of those that a mesh axis runs over, the one named last changes fastest.
Arguments:
- borders: bfloat16 [48, 512, 2048], P('scen', None, 'grp'), may hold values from -0.25 to 0.25
- row_scale: float32 [48, 512], P('scen'), may hold values from 0.1 to 10
- assign: int32 [48], P('scen'), may hold values from 0 to 47, each once
- prob: float32 [48], replicated, may hold values from 0.5 to 2
- pattern: int32 [48, 16], replicated, may hold values 0 or 1
- first_diag: float32 [2048], replicated, may hold values from 0.1 to 2
- rhs: float32 [2048], replicated, may hold values from -6 to 6
Outputs:
- schur: float32 [2048, 2048], P('scen', 'grp')
- solution: float32 [2048], replicated
The draws below stay inside these ranges and needn't reach their ends.
Inputs may be any that keep to these rules, and one draw needn't show every extreme that they name: `assign`: each scenario number appears in exactly one slot.
All inputs are finite; a program needn't handle non-finite values.
Results may differ from the reference program's by a relative error of at most 0.00053.
Values may be sent and summed in bfloat16 or wider, within the bound.
No kernel may reach another device: no remote copies, remote signals or barrier semaphores. Data moves between devices by JAX's collectives and lax.ppermute only.
A program may use at most 64 MiB of HBM per device.

```python
import math
import jax
import jax.numpy as jnp
from jax import lax

NF = 2048
R = 512
NT = 16
ITERS = 5
SC_DEV = 6
SCEN = 48
TILE = 128


def place_ends(drawn, own_key, least, high):
    spot = [jax.random.randint(jax.random.fold_in(own_key, axis), (), 0, length) for axis, length in enumerate(drawn.shape)]
    widest = drawn.shape.index(max(drawn.shape))
    next_to = spot[:widest] + [(spot[widest] + 1) % drawn.shape[widest]] + spot[widest + 1:]
    return drawn.at[tuple(spot)].set(least).at[tuple(next_to)].set(high)


def shard_levels(stream_key, extent, cuts, smallest, largest):
    level, own = 1.0, jax.random.fold_in(stream_key, 6)
    for dim, blocks in cuts:
        draws = jnp.exp(jax.random.uniform(jax.random.fold_in(own, dim), (blocks,), jnp.float32, smallest / len(cuts), largest / len(cuts)))
        level = level * jnp.repeat(draws, extent[dim] // blocks).reshape([-1 if axis == dim else 1 for axis in range(len(extent))])
    return level


def noise(rng, extent, deviation, limit, split=(), held_as=jnp.bfloat16):
    values = deviation * jax.random.normal(rng, extent, jnp.float32)
    if split:
        values = values * shard_levels(rng, extent, split, -0.22, 0.18)
    return jnp.clip(values, -limit, limit).astype(held_as)


def setup_inputs(seed: int = 0) -> dict:
    key_of = jax.random.split(jax.random.key(seed), 8)
    borders = noise(key_of[0], (SCEN, R, NF), R ** -0.5, 0.25, ((0, 8), (2, 4)))
    row_scale = jnp.clip(jnp.exp(math.log(10.0) - 4.6051702 * jax.random.uniform(key_of[1], (SCEN, R), jnp.float32) ** shard_levels(key_of[1], (SCEN, R), ((0, 8),), -0.2, 0.2)), 0.1, 10.0)
    assign = jax.random.permutation(key_of[2], SCEN).astype(jnp.int32)
    prob = jnp.clip(jnp.exp(jax.random.uniform(key_of[3], (SCEN,), jnp.float32, math.log(0.5), math.log(2.0))), 0.5, 2.0)
    pattern = place_ends((jax.random.randint(key_of[4], (SCEN, NT), 0, 4) < 3).astype(jnp.int32), jax.random.fold_in(key_of[4], 1), 0, 1)
    first_diag = jnp.clip(jnp.exp(jax.random.uniform(key_of[5], (NF,), jnp.float32, math.log(0.1), math.log(2.0))), 0.1, 2.0)
    rhs = noise(key_of[6], (NF,), 1.0, 6.0, (), jnp.float32)
    return dict(borders=borders, row_scale=row_scale, assign=assign, prob=prob, pattern=pattern, first_diag=first_diag, rhs=rhs)


def reference(borders, row_scale, assign, prob, pattern, first_diag, rhs):
    tiles_of = pattern[assign]
    col_tile = jnp.arange(NF, dtype=jnp.int32) // TILE
    keep = jnp.take(tiles_of, col_tile, axis=1).astype(borders.dtype)
    masked = borders * keep[:, None, :]
    factor = row_scale * (prob[assign] / SCEN)[:, None]
    scaled = (masked.astype(jnp.float32) * factor[:, :, None]).astype(jnp.bfloat16)
    groups = SCEN // SC_DEV
    left = masked.reshape(groups, SC_DEV * R, NF)
    right = scaled.reshape(groups, SC_DEV * R, NF)

    def accumulate(total, pair):
        one, two = pair
        term = jnp.dot(one.astype(jnp.float32).T, two.astype(jnp.float32), precision=lax.Precision.HIGHEST)
        return total + term, None

    total, unused = lax.scan(accumulate, jnp.zeros((NF, NF), jnp.float32), (left, right))
    schur = total + jnp.diag(first_diag)
    solution = jnp.zeros_like(rhs)
    residual = rhs
    direction = rhs
    norm_now = jnp.dot(residual, residual, precision=lax.Precision.HIGHEST)
    for step in range(ITERS):
        image = jnp.dot(schur, direction, precision=lax.Precision.HIGHEST)
        alpha = norm_now / jnp.dot(direction, image, precision=lax.Precision.HIGHEST)
        solution = solution + alpha * direction
        residual = residual - alpha * image
        norm_next = jnp.dot(residual, residual, precision=lax.Precision.HIGHEST)
        direction = residual + (norm_next / norm_now) * direction
        norm_now = norm_next
    return schur, solution
```

```python
import functools

import jax
import jax.numpy as jnp
from jax import lax
from jax.experimental import pallas as pl
from jax.experimental.pallas import tpu as pltpu
from jax.sharding import PartitionSpec as P

ITERS = 5
VMEM = pltpu.VMEM
SMEM = pltpu.SMEM


def split_rows(row):
    high = row.astype(jnp.bfloat16).astype(jnp.float32)
    rest = row - high
    mid = rest.astype(jnp.bfloat16).astype(jnp.float32)
    low = rest - mid
    place = lax.broadcasted_iota(jnp.int32, (8, row.shape[1]), 0)
    pieces = jnp.where(place == 0, high, jnp.where(place == 1, mid, jnp.where(place == 2, low, 0.0)))
    return pieces.astype(jnp.bfloat16)


def total(values):
    return jnp.sum(jnp.sum(values, axis=1, keepdims=True), axis=0, keepdims=True)


def row_products(grp_ref, scaled_ref, direction, out_ref):
    own = jnp.zeros_like(direction[:1])
    for j in range(direction.shape[0]):
        own = jnp.where(grp_ref[0] == j, direction[j : j + 1], own)
    pieces = split_rows(own)
    for k in range(scaled_ref.shape[0]):
        rows = scaled_ref.shape[1]
        part = lax.dot_general(
            pieces, scaled_ref[k], (((1,), (1,)), ((), ())), preferred_element_type=jnp.float32
        )
        part = jnp.sum(part, axis=0, keepdims=True)
        out_ref[:, k * rows : (k + 1) * rows] = jnp.broadcast_to(part, (out_ref.shape[0], rows))


def first_kernel(grp_ref, scaled_ref, rhs_ref, out_ref):
    row_products(grp_ref, scaled_ref, rhs_ref[...], out_ref)


def column_kernel(got_ref, raw_ref, keep_ref, out_ref):
    image = jnp.zeros((1, raw_ref.shape[2]), jnp.float32)
    rows = raw_ref.shape[1]
    for k in range(raw_ref.shape[0]):
        row = jnp.sum(got_ref[:, k * rows : (k + 1) * rows], axis=0, keepdims=True)
        part = jnp.dot(split_rows(row), raw_ref[k], preferred_element_type=jnp.float32)
        image += jnp.sum(part, axis=0, keepdims=True) * keep_ref[k : k + 1, :]
    out_ref[...] = jnp.broadcast_to(image, out_ref.shape)


def advance(got_ref, diag_ref, sol_ref, res_ref, dir_ref):
    groups = dir_ref.shape[0]
    direction, residual = dir_ref[...], res_ref[...]
    image = diag_ref[...] * direction
    for s in range(got_ref.shape[0] // groups):
        image += got_ref[s * groups : (s + 1) * groups, :]
    norm_now = total(residual * residual)
    alpha = norm_now / total(direction * image)
    solution = sol_ref[...] + alpha * direction
    residual = residual - alpha * image
    norm_next = total(residual * residual)
    return solution, residual, residual + norm_next / norm_now * direction


def step_kernel(grp_ref, scaled_ref, got_ref, diag_ref, sol_ref, res_ref, dir_ref, out_ref, sol_out, res_out, dir_out):
    solution, residual, direction = advance(got_ref, diag_ref, sol_ref, res_ref, dir_ref)
    sol_out[...], res_out[...], dir_out[...] = solution, residual, direction
    row_products(grp_ref, scaled_ref, direction, out_ref)


def last_kernel(got_ref, diag_ref, sol_ref, res_ref, dir_ref, sol_out):
    sol_out[...] = advance(got_ref, diag_ref, sol_ref, res_ref, dir_ref)[0]


def stripe_kernel(slots, left, right, grp_ref, factor_ref, keep_ref, *refs):
    raws, out_ref = refs[:-1], refs[-1]
    k = pl.program_id(0)
    cols = out_ref.shape[1]

    @pl.when(k == 0)
    def clear():
        out_ref[...] = jnp.zeros_like(out_ref)

    width = min(cols, 128)
    rows = raws[0].shape[1]
    column = jnp.transpose(jnp.broadcast_to(factor_ref[0], (width, rows)))
    column = jnp.concatenate([column] * (cols // width), axis=1)
    masked = [raw[0] * keep_ref[0, m : m + 1, :].astype(jnp.bfloat16) for m, raw in enumerate(raws)]
    scaled = {m: (masked[m].astype(jnp.float32) * column).astype(jnp.bfloat16) for m in sorted(set(right))}
    for m in range(slots):
        first = pl.multiple_of((grp_ref[0] ^ m) * cols, cols)
        out_ref[pl.ds(first, cols), :] += lax.dot_general(
            masked[left[m]], scaled[right[m]], (((0,), (0,)), ((), ())), preferred_element_type=jnp.float32
        )


def vmem_call(kernel, outs, operands, scalars=0, name=None):
    return pl.pallas_call(
        kernel,
        out_shape=outs,
        in_specs=[pl.BlockSpec(memory_space=SMEM)] * scalars
        + [pl.BlockSpec(memory_space=VMEM)] * (len(operands) - scalars),
        out_specs=jax.tree.map(lambda _: pl.BlockSpec(memory_space=VMEM), outs),
        name=name,
    )(*operands)


def scenario_tables(row_scale, assign, prob, pattern, tile_cols):
    held = assign[:, None] == jnp.arange(prob.shape[0], dtype=jnp.int32)[None, :]
    weight = jnp.sum(jnp.where(held, prob[None, :], 0.0), axis=1)
    present = jnp.sum(jnp.where(held[:, :, None], pattern[None, :, :], 0), axis=1).astype(jnp.float32)
    factor = row_scale * (weight / prob.shape[0])[:, None]
    return factor, jnp.repeat(present, tile_cols, axis=1)


def by_pairs(borders, row_scale, assign, prob, pattern, first_diag, rhs):
    slots, rows, cols = borders.shape
    groups, blocks = lax.axis_size("grp"), lax.axis_size("scen")
    full = cols * groups
    mine, block = lax.axis_index("grp"), lax.axis_index("scen")
    far = groups - 1
    near = groups // 2
    gathered = [borders] + [
        lax.ppermute(borders, "grp", [(g, g ^ m) for g in range(groups)]) for m in range(1, far)
    ]
    left = list(range(far)) + [far ^ near]
    right = [0] * far + [near]

    factor, keep = scenario_tables(row_scale, assign, prob, pattern, full // pattern.shape[1])
    keep = keep.reshape(slots, groups, cols)
    keep_of = jnp.stack(
        [lax.dynamic_index_in_dim(keep, mine ^ m, axis=1, keepdims=False) for m in range(far)], axis=1
    )
    grp_id = mine.astype(jnp.int32).reshape(1)
    own_keep = keep_of[:, 0]
    scaled = ((borders * own_keep[:, None, :].astype(jnp.bfloat16)).astype(jnp.float32) * factor[:, :, None]).astype(
        jnp.bfloat16
    )

    diag, first = first_diag.reshape(groups, cols), rhs.reshape(groups, cols)
    vec = jax.ShapeDtypeStruct((groups, cols), jnp.float32)
    wide = jax.ShapeDtypeStruct((groups, slots * rows), jnp.float32)
    image_part = jax.ShapeDtypeStruct((groups * blocks, cols), jnp.float32)
    sol, res, direction = jnp.zeros_like(first), first, first
    sent = vmem_call(first_kernel, wide, (grp_id, scaled, first), 1, "rows_first")
    for step in range(ITERS):
        got = lax.all_to_all(sent, "grp", 0, 0, tiled=True)
        part = vmem_call(column_kernel, image_part, (got, borders, own_keep), 0, "columns")
        got = lax.all_to_all(part, ("scen", "grp"), 0, 0, tiled=True)
        if step < ITERS - 1:
            sent, sol, res, direction = vmem_call(
                step_kernel, (wide, vec, vec, vec), (grp_id, scaled, got, diag, sol, res, direction), 1, "rows_next"
            )
        else:
            sol = vmem_call(last_kernel, vec, (got, diag, sol, res, direction), 0, "finish")

    stripe = pl.pallas_call(
        functools.partial(stripe_kernel, groups, left, right),
        grid=(slots,),
        in_specs=[
            pl.BlockSpec(memory_space=SMEM),
            pl.BlockSpec((1, 1, rows), lambda k: (k, 0, 0)),
            pl.BlockSpec((1, far, cols), lambda k: (k, 0, 0)),
        ]
        + [pl.BlockSpec((1, rows, cols), lambda k: (k, 0, 0))] * far,
        out_specs=pl.BlockSpec((full, cols), lambda k: (0, 0)),
        out_shape=jax.ShapeDtypeStruct((full, cols), jnp.float32),
        name="stripe",
    )(grp_id, factor.reshape(slots, 1, rows), keep_of, *gathered)

    part = lax.psum_scatter(stripe, "scen", scatter_dimension=0, tiled=True)
    moves = [
        (s * groups + g, ((g ^ far ^ near) * 2 + s % 2) * groups + (g ^ near))
        for s in range(blocks)
        for g in range(groups)
        if (s // 2) ^ g == far
    ]
    moved = lax.ppermute(part, ("scen", "grp"), moves)
    part = jnp.where((block // 2) ^ mine == far, moved, part)
    rows_blk = full // blocks
    row_ids = block * rows_blk + jnp.arange(rows_blk, dtype=jnp.int32)
    col_ids = mine * cols + jnp.arange(cols, dtype=jnp.int32)
    diag_rows = lax.dynamic_slice_in_dim(first_diag, block * rows_blk, rows_blk)
    schur = part + jnp.where(row_ids[:, None] == col_ids[None, :], diag_rows[:, None], 0.0)
    return schur, sol.reshape(full)


def by_gather(borders, row_scale, assign, prob, pattern, first_diag, rhs):
    cols = borders.shape[2]
    full = cols * lax.axis_size("grp")
    factor, keep = scenario_tables(row_scale, assign, prob, pattern, full // pattern.shape[1])
    start_col = lax.axis_index("grp") * cols
    keep = lax.dynamic_slice_in_dim(keep, start_col, cols, axis=1)
    masked = borders * keep[:, None, :].astype(jnp.bfloat16)
    scaled = (masked.astype(jnp.float32) * factor[:, :, None]).astype(jnp.bfloat16)
    stripe = jnp.einsum(
        "krm,krj->mj",
        lax.all_gather(masked, "grp", axis=2, tiled=True),
        scaled,
        preferred_element_type=jnp.float32,
    )
    rows_blk = full // lax.axis_size("scen")
    row_first = lax.axis_index("scen") * rows_blk
    row_ids = row_first + jnp.arange(rows_blk, dtype=jnp.int32)
    col_ids = start_col + jnp.arange(cols, dtype=jnp.int32)
    diag_rows = lax.dynamic_slice_in_dim(first_diag, row_first, rows_blk)
    block = lax.psum_scatter(stripe, "scen", scatter_dimension=0, tiled=True)
    schur = block + jnp.where(row_ids[:, None] == col_ids[None, :], diag_rows[:, None], 0.0)
    solution = jnp.zeros_like(rhs)
    residual = rhs
    direction = rhs
    norm_now = jnp.dot(residual, residual, precision=lax.Precision.HIGHEST)
    for step in range(ITERS):
        own = lax.dynamic_slice_in_dim(direction, start_col, cols)
        summed = lax.psum(jnp.dot(schur, own, precision=lax.Precision.HIGHEST), "grp")
        image = lax.all_gather(summed, "scen", axis=0, tiled=True)
        alpha = norm_now / jnp.dot(direction, image, precision=lax.Precision.HIGHEST)
        solution = solution + alpha * direction
        residual = residual - alpha * image
        norm_next = jnp.dot(residual, residual, precision=lax.Precision.HIGHEST)
        direction = residual + norm_next / norm_now * direction
        norm_now = norm_next
    return (schur, solution)


def solution(mesh):
    groups, blocks = mesh.shape["grp"], mesh.shape["scen"]
    paired = groups >= 4 and groups & (groups - 1) == 0 and blocks == 2 * groups
    placed = (P("scen", None, "grp"), P("scen", None), P("scen"), P(), P(), P(), P())
    return jax.shard_map(
        by_pairs if paired else by_gather,
        mesh=mesh,
        in_specs=placed,
        out_specs=(P("scen", "grp"), P()),
        check_vma=False,
    )
```

```python
import functools

import jax
import jax.numpy as jnp
from jax import lax
from jax.experimental import pallas as pl
from jax.experimental.pallas import tpu as pltpu
from jax.sharding import PartitionSpec as P


ITERS = 5
VMEM = pltpu.VMEM
SMEM = pltpu.SMEM


def split_rows(row):
    high = row.astype(jnp.bfloat16).astype(jnp.float32)
    rest = row - high
    mid = rest.astype(jnp.bfloat16).astype(jnp.float32)
    low = rest - mid
    place = lax.broadcasted_iota(jnp.int32, (8, row.shape[1]), 0)
    pieces = jnp.where(place == 0, high, jnp.where(place == 1, mid, jnp.where(place == 2, low, 0.0)))
    return pieces.astype(jnp.bfloat16)


def total(values):
    return jnp.sum(jnp.sum(values, axis=1, keepdims=True), axis=0, keepdims=True)


def keep_row(assign_ref, pattern_ref, k, part, cols, tile_cols):
    held = assign_ref[k]
    tiles = cols // tile_cols
    kept = [pattern_ref[held, part * tiles + t].astype(jnp.float32) for t in range(tiles)]
    return jnp.concatenate([jnp.full((1, tile_cols), value, jnp.float32) for value in kept], axis=1)


def factor_column(assign_ref, prob_ref, scale_row, k, cols):
    scenarios = prob_ref.shape[0]
    weight = jnp.full((1, 1), prob_ref[assign_ref[k]], jnp.float32) / scenarios
    width = min(cols, 128)
    column = jnp.transpose(jnp.broadcast_to(scale_row * weight, (width, scale_row.shape[1])))
    return jnp.concatenate([column] * (cols // width), axis=1)


def row_product(pieces, scaled):
    part = lax.dot_general(pieces, scaled, (((1,), (1,)), ((), ())), preferred_element_type=jnp.float32)
    return jnp.sum(part, axis=0, keepdims=True)


def first_kernel(tile_cols, grp_ref, assign_ref, prob_ref, pattern_ref, scale_ref, rhs_ref, raw_ref, out_ref):
    k = pl.program_id(0)
    cols = raw_ref.shape[2]
    keep = keep_row(assign_ref, pattern_ref, k, grp_ref[0], cols, tile_cols)
    masked = raw_ref[0] * keep.astype(jnp.bfloat16)
    column = factor_column(assign_ref, prob_ref, scale_ref[0], k, cols)
    scaled = (masked.astype(jnp.float32) * column).astype(jnp.bfloat16)
    part = row_product(split_rows(pick(rhs_ref[...], grp_ref[0])), scaled)
    out_ref[...] = jnp.broadcast_to(part[None], out_ref.shape)


def fetch(source_ref, held_ref, sems):
    copies = [pltpu.make_async_copy(source_ref.at[k], held_ref.at[k], sems.at[k]) for k in range(held_ref.shape[0])]
    for copy in copies:
        copy.start()
    return copies


def column_kernel(tile_cols, grp_ref, assign_ref, pattern_ref, got_ref, raw_ref, out_ref, held_ref, sems):
    copies = fetch(raw_ref, held_ref, sems)
    slots, rows, cols = held_ref.shape
    image = jnp.zeros((1, cols), jnp.float32)
    row = got_ref[0]
    for j in range(1, got_ref.shape[0]):
        row += got_ref[j]
    for k in range(slots):
        pieces = split_rows(row[:, k * rows : (k + 1) * rows])
        keep = keep_row(assign_ref, pattern_ref, k, grp_ref[0], cols, tile_cols)
        copies[k].wait()
        part = jnp.dot(pieces, held_ref[k], preferred_element_type=jnp.float32)
        image += jnp.sum(part, axis=0, keepdims=True) * keep
    out_ref[...] = jnp.broadcast_to(image[None], out_ref.shape)


def advance(got_ref, diag_ref, sol_ref, res_ref, dir_ref):
    groups, cols = dir_ref.shape
    direction, residual = dir_ref[...], res_ref[...]
    rows = [None] * groups
    for sender in range(got_ref.shape[0]):
        message = got_ref[sender]
        for m in range(message.shape[1] // cols):
            share, to = message[:, m * cols : (m + 1) * cols], (sender % groups) ^ m
            rows[to] = share if rows[to] is None else rows[to] + share
    image = diag_ref[...] * direction + jnp.concatenate(rows, axis=0)
    norm_now = total(residual * residual)
    alpha = norm_now / total(direction * image)
    solution = sol_ref[...] + alpha * direction
    residual = residual - alpha * image
    norm_next = total(residual * residual)
    return solution, residual, residual + norm_next / norm_now * direction


def pick(direction, which):
    row = jnp.zeros_like(direction[:1])
    for j in range(direction.shape[0]):
        row = jnp.where(which == j, direction[j : j + 1], row)
    return row


def step_kernel(
    near, grp_ref, got_ref, diag_ref, sol_ref, res_ref, dir_ref, stripe_ref, out_ref, sol_out, res_out, dir_out, held_ref, sems
):
    groups, cols = dir_ref.shape
    far = groups - 1
    copies = []
    for m in range(groups):
        first = pl.multiple_of((grp_ref[0] ^ m) * cols, cols)
        copies.append(pltpu.make_async_copy(stripe_ref.at[pl.ds(first, cols)], held_ref.at[m], sems.at[m]))
        copies[m].start()
    solution, residual, direction = advance(got_ref, diag_ref, sol_ref, res_ref, dir_ref)
    sol_out[...], res_out[...], dir_out[...] = solution, residual, direction
    own, other = pick(direction, grp_ref[0]), pick(direction, grp_ref[0] ^ near)
    width = min(cols, 128)

    def folded(m, first, row):
        product = held_ref[m, first : first + width, :] * row
        return sum(product[:, c : c + width] for c in range(0, cols, width))

    for copy in copies:
        copy.wait()
    for m in range(far):
        for first in range(0, cols, width):
            block = folded(m, first, own)
            if m == far ^ near:
                block += folded(far, first, other)
            part = jnp.sum(jnp.transpose(block), axis=0, keepdims=True)
            at = m * cols + first
            out_ref[:, :, at : at + width] = jnp.broadcast_to(part[None], (out_ref.shape[0], 1, width))


def last_kernel(got_ref, diag_ref, sol_ref, res_ref, dir_ref, sol_out):
    sol_out[...] = advance(got_ref, diag_ref, sol_ref, res_ref, dir_ref)[0]


def stripe_kernel(slots, left, right, tile_cols, grp_ref, assign_ref, prob_ref, pattern_ref, scale_ref, *refs):
    raws, out_ref = refs[:-1], refs[-1]
    k = pl.program_id(0)
    cols = out_ref.shape[1]

    @pl.when(k == 0)
    def clear():
        out_ref[...] = jnp.zeros_like(out_ref)

    column = factor_column(assign_ref, prob_ref, scale_ref[0], k, cols)
    masked = [
        raw[0] * keep_row(assign_ref, pattern_ref, k, grp_ref[0] ^ m, cols, tile_cols).astype(jnp.bfloat16)
        for m, raw in enumerate(raws)
    ]
    scaled = {m: (masked[m].astype(jnp.float32) * column).astype(jnp.bfloat16) for m in sorted(set(right))}
    for m in range(slots):
        first = pl.multiple_of((grp_ref[0] ^ m) * cols, cols)
        out_ref[pl.ds(first, cols), :] += lax.dot_general(
            masked[left[m]], scaled[right[m]], (((0,), (0,)), ((), ())), preferred_element_type=jnp.float32
        )


IN_VMEM = pl.BlockSpec(memory_space=VMEM)
IN_SMEM = pl.BlockSpec(memory_space=SMEM)
IN_PLACE = pl.BlockSpec(memory_space=pl.ANY)


def vector_call(kernel, outs, scalars, vectors, matrix=None, held=None):
    return pl.pallas_call(
        kernel,
        out_shape=outs,
        in_specs=[IN_SMEM] * len(scalars) + [IN_VMEM] * len(vectors) + [IN_PLACE] * (held is not None),
        out_specs=jax.tree.map(lambda _: IN_VMEM, outs),
        scratch_shapes=[] if held is None else [VMEM(*held), pltpu.SemaphoreType.DMA((held[0][0],))],
    )(*scalars, *vectors, *([] if held is None else [matrix]))


def scenario_tables(row_scale, assign, prob, pattern, tile_cols):
    held = assign[:, None] == jnp.arange(prob.shape[0], dtype=jnp.int32)[None, :]
    weight = jnp.sum(jnp.where(held, prob[None, :], 0.0), axis=1)
    present = jnp.sum(jnp.where(held[:, :, None], pattern[None, :, :], 0), axis=1).astype(jnp.float32)
    factor = row_scale * (weight / prob.shape[0])[:, None]
    return factor, jnp.repeat(present, tile_cols, axis=1)


def by_pairs(borders, row_scale, assign, prob, pattern, first_diag, rhs):
    return pair_plan(borders, row_scale, assign, prob, pattern, first_diag, rhs)


def pair_plan(borders, row_scale, assign, prob, pattern, first_diag, rhs):
    slots, rows, cols = borders.shape
    groups, blocks = lax.axis_size("grp"), lax.axis_size("scen")
    full = cols * groups
    tile_cols = full // pattern.shape[1]
    mine, block = lax.axis_index("grp"), lax.axis_index("scen")
    far = groups - 1
    near = groups // 2
    gathered = [borders]
    for m in range(1, far):
        gathered.append(lax.ppermute(borders, "grp", [(g, g ^ m) for g in range(groups)]))
    left = list(range(far)) + [far ^ near]
    right = [0] * far + [near]

    grp_id = mine.astype(jnp.int32).reshape(1)
    scale = row_scale.reshape(slots, 1, rows)
    diag, first = first_diag.reshape(groups, cols), rhs.reshape(groups, cols)
    f32 = jnp.float32
    vec = jax.ShapeDtypeStruct((groups, cols), f32)
    wide = jax.ShapeDtypeStruct((groups, 1, slots * rows), f32)
    message = lambda m: jax.ShapeDtypeStruct((groups * blocks, 1, m * cols), f32)

    one_slot = lambda k: (k, 0, 0)
    slot_specs = [pl.BlockSpec((1, 1, rows), one_slot)]
    sent = pl.pallas_call(
        functools.partial(first_kernel, tile_cols),
        grid=(slots,),
        in_specs=[IN_SMEM] * 4 + slot_specs + [IN_VMEM, pl.BlockSpec((1, rows, cols), one_slot)],
        out_specs=pl.BlockSpec((groups, 1, rows), lambda k: (0, 0, k)),
        out_shape=wide,
        name="rows_first",
    )(grp_id, assign, prob, pattern, scale, first, borders)
    got = lax.all_to_all(sent, "grp", 0, 0, tiled=True)
    part = vector_call(
        functools.partial(column_kernel, tile_cols),
        message(1),
        (grp_id, assign, pattern),
        (got,),
        borders,
        (borders.shape, borders.dtype),
    )
    got = lax.all_to_all(part, ("scen", "grp"), 0, 0, tiled=True)

    stripe = pl.pallas_call(
        functools.partial(stripe_kernel, groups, left, right, tile_cols),
        grid=(slots,),
        in_specs=[IN_SMEM] * 4 + slot_specs + [pl.BlockSpec((1, rows, cols), one_slot)] * far,
        out_specs=pl.BlockSpec((full, cols), lambda k: (0, 0)),
        out_shape=jax.ShapeDtypeStruct((full, cols), f32),
        name="stripe",
    )(grp_id, assign, prob, pattern, scale, *gathered)

    sol, res, direction = jnp.zeros_like(first), first, first
    for _ in range(1, ITERS):
        sent, sol, res, direction = vector_call(
            functools.partial(step_kernel, near),
            (message(far), vec, vec, vec),
            (grp_id,),
            (got, diag, sol, res, direction),
            stripe,
            ((groups, cols, cols), f32),
        )
        got = lax.all_to_all(sent, ("scen", "grp"), 0, 0, tiled=True)
    sol = vector_call(last_kernel, vec, (), (got, diag, sol, res, direction))

    part = lax.psum_scatter(stripe, "scen", scatter_dimension=0, tiled=True)
    moves = [
        (s * groups + g, ((g ^ far ^ near) * 2 + s % 2) * groups + (g ^ near))
        for s in range(blocks)
        for g in range(groups)
        if (s // 2) ^ g == far
    ]
    moved = lax.ppermute(part, ("scen", "grp"), moves)
    part = jnp.where((block // 2) ^ mine == far, moved, part)
    rows_blk = full // blocks
    row_ids = block * rows_blk + jnp.arange(rows_blk, dtype=jnp.int32)
    col_ids = mine * cols + jnp.arange(cols, dtype=jnp.int32)
    diag_rows = lax.dynamic_slice_in_dim(first_diag, block * rows_blk, rows_blk)
    schur = part + jnp.where(row_ids[:, None] == col_ids[None, :], diag_rows[:, None], 0.0)
    return schur, sol.reshape(full)


def by_gather(borders, row_scale, assign, prob, pattern, first_diag, rhs):
    cols = borders.shape[2]
    full = cols * lax.axis_size("grp")
    factor, keep = scenario_tables(row_scale, assign, prob, pattern, full // pattern.shape[1])
    start_col = lax.axis_index("grp") * cols
    keep = lax.dynamic_slice_in_dim(keep, start_col, cols, axis=1)
    masked = borders * keep[:, None, :].astype(jnp.bfloat16)
    scaled = (masked.astype(jnp.float32) * factor[:, :, None]).astype(jnp.bfloat16)
    stripe = jnp.einsum(
        "krm,krj->mj",
        lax.all_gather(masked, "grp", axis=2, tiled=True),
        scaled,
        preferred_element_type=jnp.float32,
    )
    rows_blk = full // lax.axis_size("scen")
    row_first = lax.axis_index("scen") * rows_blk
    row_ids = row_first + jnp.arange(rows_blk, dtype=jnp.int32)
    col_ids = start_col + jnp.arange(cols, dtype=jnp.int32)
    diag_rows = lax.dynamic_slice_in_dim(first_diag, row_first, rows_blk)
    block = lax.psum_scatter(stripe, "scen", scatter_dimension=0, tiled=True)
    schur = block + jnp.where(row_ids[:, None] == col_ids[None, :], diag_rows[:, None], 0.0)
    solution = jnp.zeros_like(rhs)
    residual = rhs
    direction = rhs
    norm_now = jnp.dot(residual, residual, precision=lax.Precision.HIGHEST)
    for _ in range(ITERS):
        own = lax.dynamic_slice_in_dim(direction, start_col, cols)
        summed = lax.psum(jnp.dot(schur, own, precision=lax.Precision.HIGHEST), "grp")
        image = lax.all_gather(summed, "scen", axis=0, tiled=True)
        alpha = norm_now / jnp.dot(direction, image, precision=lax.Precision.HIGHEST)
        solution = solution + alpha * direction
        residual = residual - alpha * image
        norm_next = jnp.dot(residual, residual, precision=lax.Precision.HIGHEST)
        direction = residual + norm_next / norm_now * direction
        norm_now = norm_next
    return (schur, solution)


def solution(mesh):
    groups, blocks = mesh.shape["grp"], mesh.shape["scen"]
    paired = groups >= 4 and groups & (groups - 1) == 0 and blocks == 2 * groups
    placed = (P("scen", None, "grp"), P("scen", None), P("scen"), P(), P(), P(), P())
    return jax.shard_map(
        by_pairs if paired else by_gather,
        mesh=mesh,
        in_specs=placed,
        out_specs=(P("scen", "grp"), P()),
        check_vma=False,
    )
```
